32 devices in a mesh: row: 4 (over x, core), col: 8 (over z, y).
Axes of the slice: x: 2, y: 2, z: 4, core: 2. Of those that a mesh axis runs over, the one named last changes fastest.
Arguments:
- momentum: bfloat16 [8704, 30720], P('row', 'col'), may hold values from -6 to 6
- grad: bfloat16 [8704, 30720], P('row', 'col'), may hold values from -6 to 6
- q_prev: bfloat16 [30720, 512], P('col'), may hold values from -6 to 6
- row_counts: int32 [4], replicated, may hold values from 1 to 17, 64 in all
- col_counts: int32 [8], replicated, may hold values from 1 to 30, 224 in all
Outputs:
- momentum_out: bfloat16 [8704, 30720], P('row', 'col')
- basis_out: bfloat16 [30720, 512], P('col')
- update: bfloat16 [8704, 30720], P('row', 'col')
The draws below stay inside these ranges and needn't reach their ends.
Inputs may be any that keep to these rules, and one draw needn't show every extreme that they name: `row_counts`: each index of row holds 1 to 17 live row blocks, the counts sum to 64, and some index holds exactly 17; live blocks are the first slots of a device. `col_counts`: each index of col holds 1 to 30 live column blocks, the counts sum to 224, and some index holds exactly 30; live blocks are the first slots of a device.
All inputs are finite; a program needn't handle non-finite values.
Results may differ from the reference program's by a relative error of at most 0.0079.
Values may be sent and summed in bfloat16 or wider, within the bound.
No kernel may reach another device: no remote copies, remote signals or barrier semaphores. Data moves between devices by JAX's collectives and lax.ppermute only.
A program may use at most 128 MiB of HBM per device.

```python
import math
import jax
import jax.numpy as jnp
import numpy as np
from jax import lax

D = 8192
FF = 28672
RANK = 512
BLOCK = 128
ROW_BLOCKS = 64
COL_BLOCKS = 224
CAP_R = 17
CAP_C = 30
MROWS = 8704
MCOLS = 30720
N_ROW = 4
N_COL = 8


def block_scale(rng, dims, shards, least, largest):
    loudness, own = 1.0, jax.random.fold_in(rng, 6)
    for axis_at, parts in shards:
        draws = jnp.exp(jax.random.uniform(jax.random.fold_in(own, axis_at), (parts,), jnp.float32, least / len(shards), largest / len(shards)))
        loudness = loudness * jnp.repeat(draws, dims[axis_at] // parts).reshape([-1 if axis == axis_at else 1 for axis in range(len(dims))])
    return loudness


def profile(count, total, reach, lean):
    loads = [(1 << 20) // math.isqrt(rank ** lean) + 1 for rank in range(2, count + 1)]
    surplus, given = total - reach - (count - 1), [1] * (count - 1)
    while surplus > 0:
        movable = [i for i in range(count - 1) if given[i] < reach]
        pool, budget = sum([loads[i] for i in movable]), surplus
        for i in movable:
            more = min(reach - given[i], max(1, budget * loads[i] // pool), surplus)
            given[i] = given[i] + more
            surplus = surplus - more
    return np.array([reach] + given)


def uneven(rng, count, total, bound, slope):
    if count == 2:
        one = jax.random.randint(rng, (), max(1, total - bound), min(bound, total - 1) + 1)
        return jnp.stack([one, total - one])
    lengths = jnp.asarray(profile(count, total, bound, slope), jnp.int32)
    twos = (count - 1) // 2
    donor, sink = lengths[1:1 + 2 * twos:2], lengths[2:2 + 2 * twos:2]
    room = jnp.minimum(donor - 1, bound - sink)
    moved = jax.random.randint(jax.random.fold_in(rng, 1), (twos,), 0, 1 << 20) % (room + 1)
    lengths = lengths.at[1:1 + 2 * twos:2].set(donor - moved).at[2:2 + 2 * twos:2].set(sink + moved)
    return lengths[jax.random.permutation(jax.random.fold_in(rng, 2), count)]


def normal_values(key, extent, deviation, most, split=(), kind=jnp.bfloat16):
    entries = deviation * jax.random.normal(key, extent, jnp.float32)
    if split:
        entries = entries * block_scale(key, extent, split, -0.22, 0.18)
    return jnp.clip(entries, -most, most).astype(kind)


def setup_inputs(seed: int = 0) -> dict:
    arg_keys = jax.random.split(jax.random.key(seed), 6)
    momentum = normal_values(arg_keys[0], (MROWS, MCOLS), 1.0, 6.0, ((0, 4), (1, 8)))
    grad = normal_values(arg_keys[1], (MROWS, MCOLS), 1.0, 6.0, ((0, 4), (1, 8)))
    q_prev = normal_values(arg_keys[2], (MCOLS, RANK), 1.0, 6.0, ((0, 8),))
    row_counts = uneven(arg_keys[3], N_ROW, ROW_BLOCKS, CAP_R, 2).astype(jnp.int32)
    col_counts = uneven(arg_keys[4], N_COL, COL_BLOCKS, CAP_C, 2).astype(jnp.int32)
    return dict(momentum=momentum, grad=grad, q_prev=q_prev, row_counts=row_counts, col_counts=col_counts)


EPS = 1e-06
ERR = 0.05

def slot_mask(counts, slots):
    inside = jnp.arange(slots * BLOCK, dtype=jnp.int32)[None, :] < counts[:, None] * BLOCK
    return inside.reshape(-1)

def tri_inverse(gram_matrix):
    lower_factor = jnp.linalg.cholesky(gram_matrix)
    ident = jnp.eye(gram_matrix.shape[0], dtype=gram_matrix.dtype)
    return jax.scipy.linalg.solve_triangular(lower_factor, ident, lower=True)

def reference(momentum, grad, q_prev, row_counts, col_counts):
    row_mask = slot_mask(row_counts, CAP_R)
    col_mask = slot_mask(col_counts, CAP_C)
    summed = (momentum.astype(jnp.float32) + grad.astype(jnp.float32)).astype(jnp.bfloat16)
    buffer = jnp.where(row_mask[:, None] & col_mask[None, :], summed, jnp.zeros((), jnp.bfloat16))
    prev_basis = jnp.where(col_mask[:, None], q_prev, jnp.zeros((), jnp.bfloat16))
    left_part = jnp.dot(buffer.astype(jnp.float32), prev_basis.astype(jnp.float32), preferred_element_type=jnp.float32)
    gram_matrix = jnp.dot(left_part.T, left_part, precision=lax.Precision.HIGHEST)
    inverse = tri_inverse(gram_matrix)
    ortho = jnp.dot(left_part, inverse.T, precision=lax.Precision.HIGHEST).astype(jnp.bfloat16)
    right_part = lax.dot_general(buffer.astype(jnp.float32), ortho.astype(jnp.float32), (((0,), (0,)), ((), ())), preferred_element_type=jnp.float32)
    squares = lax.optimization_barrier(jnp.sum(right_part * right_part, axis=0))
    norm_factor = lax.rsqrt(squares / FF + EPS)
    right_b = right_part.astype(jnp.bfloat16)
    basis_out = (right_part * norm_factor[None, :]).astype(jnp.bfloat16)
    feedback = lax.dot_general(ortho.astype(jnp.float32), right_b.astype(jnp.float32), (((1,), (1,)), ((), ())), preferred_element_type=jnp.float32)
    momentum_out = (buffer.astype(jnp.float32) - ERR * feedback).astype(jnp.bfloat16)
    direction = lax.dot_general(ortho.astype(jnp.float32), basis_out.astype(jnp.float32), (((1,), (1,)), ((), ())), preferred_element_type=jnp.float32)
    update = (math.sqrt(D / RANK) * direction).astype(jnp.bfloat16)
    return (momentum_out, basis_out, update)
```

```python
import math

import jax
import jax.numpy as jnp
from jax import lax
from jax.experimental import pallas as pl
from jax.experimental.pallas import tpu as pltpu
from jax.sharding import PartitionSpec as P

D = 8192
FF = 28672
RANK = 512
BLOCK = 128


EPS = 1e-06
ERR = 0.05


HIGHEST = lax.Precision.HIGHEST
TILE = 128
SUB = 8


def matmul(left, right, contract):
    return lax.dot_general(
        left, right, (contract, ((), ())), precision=HIGHEST, preferred_element_type=jnp.float32
    )


def tile_inverse(rows, size):
    groups = size // SUB
    sub = lax.broadcasted_iota(jnp.int32, (SUB, size), 0)
    lane = lax.broadcasted_iota(jnp.int32, (SUB, size), 1)
    inv = [jnp.where(lane == sub + SUB * g, 1.0, 0.0) for g in range(groups)]
    for j in range(size):
        g0, s = divmod(j, SUB)
        row = rows[g0][s : s + 1, :]
        pivot = jnp.broadcast_to(row[:, j : j + 1], (1, size))
        scale = lax.rsqrt(pivot)
        scale = scale * (1.5 - 0.5 * pivot * scale * scale)
        low_row = row * scale
        inv_row = inv[g0][s : s + 1, :] * scale
        low_times = low_row * scale
        inv_times = inv_row * scale
        for g in range(g0, groups):
            factor = jnp.broadcast_to(rows[g][:, j : j + 1], (SUB, size))
            if g == g0:
                factor = jnp.where(sub > s, factor, 0.0)
                inv[g] = jnp.where(sub == s, inv_row, inv[g] - factor * inv_times)
            else:
                inv[g] = inv[g] - factor * inv_times
            rows[g] = rows[g] - factor * low_times
    return jnp.concatenate(inv, axis=0)


def inverse_kernel(gram_ref, out_ref, work_ref):
    rank = gram_ref.shape[0]
    work_ref[...] = gram_ref[...]
    row_id = lax.broadcasted_iota(jnp.int32, (rank, rank), 0)
    col_id = lax.broadcasted_iota(jnp.int32, (rank, rank), 1)
    out_ref[...] = jnp.where(row_id == col_id, 1.0, 0.0)

    def step(k, carry):
        base = pl.multiple_of(k * TILE, TILE)
        here = pl.ds(base, TILE)
        rows = [
            work_ref[pl.ds(pl.multiple_of(base + SUB * g, SUB), SUB), here]
            for g in range(TILE // SUB)
        ]
        tile_inv = tile_inverse(rows, TILE)
        panel = matmul(work_ref[:, here], tile_inv, ((1,), (1,)))
        below = lax.broadcasted_iota(jnp.int32, (rank, TILE), 0) >= base + TILE
        panel = jnp.where(below, panel, 0.0)
        solved = matmul(tile_inv, out_ref[here, :], ((1,), (0,)))
        work_ref[...] = work_ref[...] - matmul(panel, panel, ((1,), (1,)))
        out_ref[...] = out_ref[...] - matmul(panel, solved, ((1,), (0,)))
        out_ref[here, :] = solved
        return carry

    lax.fori_loop(0, rank // TILE, step, 0)


def tri_inverse(gram_matrix):
    return pl.pallas_call(
        inverse_kernel,
        out_shape=jax.ShapeDtypeStruct(gram_matrix.shape, jnp.float32),
        scratch_shapes=[pltpu.VMEM(gram_matrix.shape, jnp.float32)],
    )(gram_matrix)


def on_device(momentum, grad, q_prev, row_counts, col_counts):
    row_slots, col_slots = momentum.shape
    row_live = row_counts[lax.axis_index("row")] * BLOCK
    col_live = col_counts[lax.axis_index("col")] * BLOCK
    row_mask = jnp.arange(row_slots, dtype=jnp.int32) < row_live
    col_mask = jnp.arange(col_slots, dtype=jnp.int32) < col_live
    summed = (momentum.astype(jnp.float32) + grad.astype(jnp.float32)).astype(jnp.bfloat16)
    buffer = jnp.where(row_mask[:, None] & col_mask[None, :], summed, jnp.zeros((), jnp.bfloat16))
    prev_basis = jnp.where(col_mask[:, None], q_prev, jnp.zeros((), jnp.bfloat16))
    partial_left = jnp.dot(buffer, prev_basis, preferred_element_type=jnp.float32)
    left_part = lax.psum_scatter(partial_left, "col", scatter_dimension=0, tiled=True)
    gram_local = jnp.dot(left_part.T, left_part, precision=HIGHEST)
    gram_matrix = lax.psum(gram_local, ("row", "col"))
    inverse = tri_inverse(gram_matrix)
    ortho_piece = jnp.dot(left_part, inverse.T, precision=HIGHEST).astype(jnp.bfloat16)
    ortho = lax.all_gather(ortho_piece, "col", axis=0, tiled=True)
    right_local = lax.dot_general(
        buffer, ortho, (((0,), (0,)), ((), ())), preferred_element_type=jnp.float32
    )
    right_piece = lax.psum_scatter(
        right_local.astype(jnp.bfloat16), "row", scatter_dimension=0, tiled=True
    )
    right_b = lax.all_gather(right_piece, "row", axis=0, tiled=True)
    right_part = right_piece.astype(jnp.float32)
    squares = lax.psum(jnp.sum(right_part * right_part, axis=0), ("row", "col"))
    norm_factor = lax.rsqrt(squares / FF + EPS)
    basis_out = (right_b.astype(jnp.float32) * norm_factor[None, :]).astype(jnp.bfloat16)
    feedback = lax.dot_general(
        ortho, right_b, (((1,), (1,)), ((), ())), preferred_element_type=jnp.float32
    )
    momentum_out = (buffer.astype(jnp.float32) - ERR * feedback).astype(jnp.bfloat16)
    direction = lax.dot_general(
        ortho, basis_out, (((1,), (1,)), ((), ())), preferred_element_type=jnp.float32
    )
    update = (math.sqrt(D / RANK) * direction).astype(jnp.bfloat16)
    return (momentum_out, basis_out, update)


def solution(mesh):
    placed = (P("row", "col"), P("row", "col"), P("col", None), P(), P())
    return jax.shard_map(
        on_device,
        mesh=mesh,
        in_specs=placed,
        out_specs=(P("row", "col"), P("col", None), P("row", "col")),
        check_vma=False,
    )
```
